64 devices in a mesh: dp: 4 (over x, y), sp: 16 (over z, core).
Axes of the slice: x: 2, y: 2, z: 8, core: 2. Of those that a mesh axis runs over, the one named last changes fastest.
The devices are a block of a 4x4x8 slice.
Arguments:
- q: bfloat16 [128, 56, 128], P('dp'), parts along dimension 0
- k: bfloat16 [128, 8192, 8, 128], P('dp', 'sp'), parts along dimension 0
- v: bfloat16 [128, 8192, 8, 128], P('dp', 'sp'), parts along dimension 0
Outputs:
- q: bfloat16 [128, 56, 128], P('dp'), parts along dimension 0
There are 4 independent parts. The reference program is written for one: setup_inputs(seed, part) draws one part's arguments, and reference() takes and returns one part's arrays. A program takes and returns all parts, laid end to end along the dimension named above; each array names one.
All inputs are finite; a program needn't handle non-finite values.
Results may differ from the reference program's by a relative error of at most 0.012.
Values are sent between devices in bfloat16 or wider.
A program may use at most 768 MiB of HBM per device.

```python
import jax
import jax.numpy as jnp

BATCH = 32
CACHE = 8192
HEADS = 56
KV_HEADS = 8
HEAD = 128


def setup_inputs(seed: int = 0, part: int = 0) -> dict:
    kq, kk, kv = (jax.random.fold_in(k, part) for k in jax.random.split(jax.random.key(seed), 3))
    return {
        "q": (3 * jax.random.normal(kq, (BATCH, HEADS, HEAD), jnp.float32)).astype(jnp.bfloat16),
        "k": jax.random.normal(kk, (BATCH, CACHE, KV_HEADS, HEAD), jnp.float32).astype(jnp.bfloat16),
        "v": jax.random.normal(kv, (BATCH, CACHE, KV_HEADS, HEAD), jnp.float32).astype(jnp.bfloat16),
    }


def einsum(form, a, b):
    return jnp.einsum(form, a.astype(jnp.float32), b.astype(jnp.float32))


def reference(q, k, v):
    grouped = q.reshape(BATCH, KV_HEADS, -1, HEAD)
    scores = einsum("bgsd,bugd->bgsu", grouped, k) * HEAD**-0.5
    weights = jax.nn.softmax(scores, -1).astype(jnp.bfloat16)
    return einsum("bgsu,bugd->bgsd", weights, v).astype(jnp.bfloat16).reshape(BATCH, HEADS, HEAD)
```

```python
import functools
import math

import jax
import jax.numpy as jnp
from jax import lax
from jax.experimental import pallas as pl
from jax.experimental.pallas import tpu as pltpu
from jax.sharding import PartitionSpec as P

F32, BF16 = jnp.float32, jnp.bfloat16
MESH = pl.DeviceIdType.MESH
SLOTS = 5
CHUNK = 512
LANES = 128


def kernel(n, key_heads, q_hbm, k_hbm, v_hbm, o_ref, qv, kbuf, vbuf, s0, s1, qb0, qb1, stage, stage_ml, own_f, recv, recv_ml,
           qsem, ksem, vsem, osend, orecv, msend, mrecv, gsend, grecv):
    seqs, heads, head = qv.shape
    rounds = seqs // n
    rep = heads // key_heads
    side = LANES // 2
    half = kbuf.shape[1] // 2
    pieces = half // CHUNK
    scale = head**-0.5 * math.log2(math.e)
    me = lax.axis_index("sp")

    def owner(step):
        t = lax.rem(step, n)
        u, chips = t // 2, n // 2
        odd = lax.rem(u, 2)
        dz = chips // 2 + (u // 2) * (1 - odd) - ((u + 1) // 2) * odd
        z = lax.rem(me // 2 + dz, chips)
        core = lax.rem(lax.rem(me, 2) + 1 + t, 2)
        return 2 * z + core

    def sequence(step):
        return (step // n) * n + owner(step)

    def kcopy(step):
        slot = lax.rem(step, SLOTS)
        return pltpu.make_async_copy(k_hbm.at[sequence(step)], kbuf.at[slot], ksem.at[slot])

    def vcopy(step):
        slot = lax.rem(step, SLOTS)
        return pltpu.make_async_copy(v_hbm.at[sequence(step)], vbuf.at[slot], vsem.at[slot])

    def part_copies(step):
        to, r = owner(step), step // n
        return (
            pltpu.make_async_remote_copy(stage.at[step], recv.at[r, me], osend.at[step], orecv.at[r, me], device_id={"sp": to}, device_id_type=MESH),
            pltpu.make_async_remote_copy(stage_ml.at[step], recv_ml.at[r, me], msend.at[step], mrecv.at[r, me], device_id={"sp": to}, device_id_type=MESH),
        )

    def part_arrivals(r, source):
        return (
            pltpu.make_async_remote_copy(stage.at[0], recv.at[r, source], osend.at[0], orecv.at[r, source], device_id={"sp": source}, device_id_type=MESH),
            pltpu.make_async_remote_copy(stage_ml.at[0], recv_ml.at[r, source], msend.at[0], mrecv.at[r, source], device_id={"sp": source}, device_id_type=MESH),
        )

    def result_copy(r, to):
        at = r * n + me
        return pltpu.make_async_remote_copy(o_ref.at[at], o_ref.at[at], gsend.at[r, to], grecv.at[r, me], device_id={"sp": to}, device_id_type=MESH)

    def result_arrival(r, source):
        at = r * n + source
        return pltpu.make_async_remote_copy(o_ref.at[at], o_ref.at[at], gsend.at[r, source], grecv.at[r, source], device_id={"sp": source}, device_id_type=MESH)

    kcopy(0).start()
    qcopy = pltpu.make_async_copy(q_hbm, qv, qsem)
    qcopy.start()
    vcopy(0).start()
    for step in range(1, SLOTS):
        kcopy(step).start()
        vcopy(step).start()
    barrier = pltpu.get_barrier_semaphore()
    for far in range(1, n):
        pl.semaphore_signal(barrier, inc=1, device_id={"sp": lax.rem(me + far, n)}, device_id_type=MESH)
    for qb in (qb0, qb1):
        qb[...] = jnp.zeros(qb.shape, qb.dtype)
    for r in range(rounds):
        recv[r, me] = jnp.zeros((heads, head), BF16)

    def own_mask(rows):
        row = lax.rem(lax.broadcasted_iota(jnp.int32, (rows, LANES), 0), key_heads)
        lane = lax.rem(lax.broadcasted_iota(jnp.int32, (rows, LANES), 1), side)
        return (lane >= row * rep) & (lane < row * rep + rep)

    own8, own16 = own_mask(8), own_mask(16)

    def scores_start(step, qb):
        kcopy(step).wait()
        queries = qv[sequence(step)]
        qb[0:heads, 0:head] = queries
        qb[side : side + heads, head : 2 * head] = queries

    def scores_piece(step, piece, qb, s, high):
        slot = lax.rem(step, SLOTS)
        keys = jnp.concatenate([kbuf[slot, pl.ds(piece * CHUNK, CHUNK), :], kbuf[slot, pl.ds(half + piece * CHUNK, CHUNK), :]], axis=1)
        scores = lax.dot_general(keys, qb[...], (((1,), (1,)), ((), ())), preferred_element_type=F32)
        s[pl.ds(piece * CHUNK, CHUNK), :] = scores
        return jnp.maximum(high, jnp.max(scores.reshape(CHUNK // 8, 8, LANES), axis=0))

    def scores_end(high):
        high = jnp.max(jnp.where(own8, high, -jnp.inf), axis=0, keepdims=True)
        return jnp.maximum(high, pltpu.roll(high, side, 1))

    def values_piece(step, piece, s, high, total, seen):
        slot = lax.rem(step, SLOTS)
        weights = jnp.exp2(s[pl.ds(piece * CHUNK, CHUNK), :] * scale - high * scale)
        total = total + jnp.sum(weights.reshape(CHUNK // 8, 8, LANES), axis=0)
        rounded = weights.astype(BF16).reshape(CHUNK // 16, 16, LANES)
        rounded = jnp.where(own16[None], rounded, jnp.zeros_like(rounded)).reshape(CHUNK, LANES)
        values = jnp.concatenate([vbuf[slot, pl.ds(piece * CHUNK, CHUNK), :], vbuf[slot, pl.ds(half + piece * CHUNK, CHUNK), :]], axis=1)
        return total, seen + lax.dot_general(rounded, values, (((0,), (0,)), ((), ())), preferred_element_type=F32)

    def values_end(step, high, total, seen):
        total = jnp.sum(jnp.where(own8, total, 0.0), axis=0, keepdims=True)
        total = total + pltpu.roll(total, side, 1)
        seen = seen[0:heads, 0:head] + seen[side : side + heads, head : 2 * head]
        stage[step] = seen.astype(BF16)
        own_f[step // n] = seen
        stage_ml[step] = jnp.concatenate([high, total], axis=0)

    first = jnp.full((8, LANES), -jnp.inf, F32)
    zeros = (jnp.zeros((8, LANES), F32), jnp.zeros((2 * side, 2 * head), F32))

    def send(step):
        @pl.when(lax.rem(step, n) != n - 1)
        def _():
            for copy in part_copies(step):
                copy.start()

    def both(step, high, qb, s, s_before):
        scores_start(step, qb)
        vcopy(step - 1).wait()
        new, (total, seen) = first, zeros
        for piece in range(pieces):
            new = scores_piece(step, piece, qb, s, new)
            total, seen = values_piece(step - 1, piece, s_before, high, total, seen)
        values_end(step - 1, high, total, seen)
        return scores_end(new)

    def refill(step):
        @pl.when(step + SLOTS < seqs)
        def _():
            kcopy(step + SLOTS).start()

        @pl.when(step - 1 + SLOTS < seqs)
        def _():
            vcopy(step - 1 + SLOTS).start()

    def combine(r):
        recv_ml[r, me] = stage_ml[r * n + n - 1]
        for far in range(1, n):
            for copy in part_arrivals(r, lax.rem(me + far, n)):
                copy.wait_recv()
        high, total = recv_ml[r, :, 0, :], recv_ml[r, :, 1, :]
        highest = jnp.max(high, axis=0, keepdims=True)
        share = jnp.exp2(high * scale - highest * scale)
        whole = jnp.sum(share * total, axis=0, keepdims=True)
        mine = jnp.exp2(stage_ml[r * n + n - 1, 0:1, :] * scale - highest * scale)
        share = jnp.concatenate([share, jnp.broadcast_to(mine, (8, LANES))], axis=0) / whole
        share = jnp.concatenate([share, jnp.zeros((LANES - n - 8, LANES), F32)], axis=0).T
        result = share[0:heads, n : n + 1] * own_f[r]
        for source in range(n):
            result = result + share[0:heads, source : source + 1] * recv[r, source].astype(F32)
        o_ref[r * n + me] = result.astype(BF16)
        for far in range(1, n):
            result_copy(r, lax.rem(me + far, n)).start()

    qcopy.wait()
    scores_start(0, qb0)
    high = first
    for piece in range(pieces):
        high = scores_piece(0, piece, qb0, s0, high)
    high = scores_end(high)
    kcopy(SLOTS).start()
    pl.semaphore_wait(barrier, n - 1)

    def body(trip, high):
        step = 2 * trip + 1
        high = both(step, high, qb1, s1, s0)
        refill(step)

        @pl.when(trip >= 1)
        def _():
            send(step - 2)

        high = both(step + 1, high, qb0, s0, s1)
        refill(step + 1)
        send(step - 1)
        for r in range(rounds - 1):
            @pl.when(step + 1 == (r + 1) * n + 4)
            def _():
                combine(r)

        return high

    high = lax.fori_loop(0, (seqs - 2) // 2, body, high)
    send(seqs - 3)
    high = both(seqs - 1, high, qb1, s1, s0)
    send(seqs - 2)
    vcopy(seqs - 1).wait()
    total, seen = zeros
    for piece in range(pieces):
        total, seen = values_piece(seqs - 1, piece, s1, high, total, seen)
    values_end(seqs - 1, high, total, seen)
    combine(rounds - 1)

    def drain(step, _):
        @pl.when(lax.rem(step, n) != n - 1)
        def _():
            for copy in part_copies(step):
                copy.wait_send()

        return 0

    lax.fori_loop(0, seqs, drain, 0)
    for r in range(rounds):
        for far in range(1, n):
            other = lax.rem(me + far, n)
            result_copy(r, other).wait_send()
            result_arrival(r, other).wait_recv()


def solution(mesh):
    n = mesh.shape["sp"]

    def step(q, k, v):
        seqs, heads, head = q.shape
        tokens, key_heads = k.shape[1:3]
        rows = tokens * key_heads
        rounds = seqs // n
        anywhere = pl.BlockSpec(memory_space=pl.ANY)
        dma = pltpu.SemaphoreType.DMA
        return pl.pallas_call(
            functools.partial(kernel, n, key_heads),
            out_shape=jax.ShapeDtypeStruct(q.shape, BF16),
            in_specs=[anywhere] * 3,
            out_specs=pl.BlockSpec(memory_space=pltpu.VMEM),
            scratch_shapes=[
                pltpu.VMEM(q.shape, BF16),
                pltpu.VMEM((SLOTS, rows, head), BF16),
                pltpu.VMEM((SLOTS, rows, head), BF16),
                pltpu.VMEM((rows // 2, LANES), F32),
                pltpu.VMEM((rows // 2, LANES), F32),
                pltpu.VMEM((LANES, 2 * head), BF16),
                pltpu.VMEM((LANES, 2 * head), BF16),
                pltpu.VMEM((seqs, heads, head), BF16),
                pltpu.VMEM((seqs, 2, LANES), F32),
                pltpu.VMEM((rounds, heads, head), F32),
                pltpu.VMEM((rounds, n, heads, head), BF16),
                pltpu.VMEM((rounds, n, 2, LANES), F32),
                dma,
                dma((SLOTS,)),
                dma((SLOTS,)),
                dma((seqs,)),
                dma((rounds, n)),
                dma((seqs,)),
                dma((rounds, n)),
                dma((rounds, n)),
                dma((rounds, n)),
            ],
            compiler_params=pltpu.CompilerParams(collective_id=0, has_side_effects=True, vmem_limit_bytes=40 << 20),
        )(q, k.reshape(seqs, rows, head), v.reshape(seqs, rows, head))

    return jax.shard_map(
        step,
        mesh=mesh,
        in_specs=(P("dp", None, None), P("dp", "sp", None, None), P("dp", "sp", None, None)),
        out_specs=P("dp", None, None),
        check_vma=False,
    )
```

```python
import functools
import math

import jax
import jax.numpy as jnp
from jax import lax
from jax.experimental import pallas as pl
from jax.experimental.pallas import tpu as pltpu
from jax.sharding import PartitionSpec as P

F32, BF16 = jnp.float32, jnp.bfloat16
MESH = pl.DeviceIdType.MESH
SLOTS = 8
CHUNK = 1024
LANES = 128


def kernel(n, key_heads, q_hbm, k_hbm, v_hbm, o_ref, qv, kbuf, vbuf, s0, s1, qb0, qb1, stage, stage_ml, own_f, recv, recv_ml,
           qsem, ksem, vsem, osend, orecv, msend, mrecv, gsend, grecv, fsend, frecv):
    seqs, heads, head = qv.shape
    rounds = seqs // n
    rep = heads // key_heads
    side = LANES // 2
    half = kbuf.shape[1] // 2
    pieces = half // CHUNK
    scale = head**-0.5 * math.log2(math.e)
    me = lax.axis_index("sp")

    chips = n // 2
    partner = 2 * (me // 2) + 1 - lax.rem(me, 2)

    def ahead(u):
        odd = u % 2
        return chips // 2 + (u // 2) * (1 - odd) - ((u + 1) // 2) * odd

    def device(dz, other):
        return 2 * lax.rem(me // 2 + dz, chips) + lax.rem(lax.rem(me, 2) + other, 2)

    def owner(step):
        t = lax.rem(step, n)
        return device(ahead(t // 2), 1 - lax.rem(t, 2))

    def sequence(step):
        return (step // n) * n + owner(step)

    def kcopy(step):
        slot = lax.rem(step, SLOTS)
        return pltpu.make_async_copy(k_hbm.at[sequence(step)], kbuf.at[slot], ksem.at[slot])

    def vcopy(step):
        slot = lax.rem(step, SLOTS)
        return pltpu.make_async_copy(v_hbm.at[sequence(step)], vbuf.at[slot], vsem.at[slot])

    def part_copies(step):
        to, r, t = owner(step), step // n, lax.rem(step, n)
        return (
            pltpu.make_async_remote_copy(stage.at[step], recv.at[r, t], osend.at[step], orecv.at[r, t], device_id={"sp": to}, device_id_type=MESH),
            pltpu.make_async_remote_copy(stage_ml.at[step], recv_ml.at[r, t], msend.at[step], mrecv.at[r, t], device_id={"sp": to}, device_id_type=MESH),
        )

    def result_copy(r, u):
        at = r * n + me
        to = device(ahead(u), 0) if u < chips - 1 else partner
        return pltpu.make_async_remote_copy(o_ref.at[at], o_ref.at[at], gsend.at[r, u], grecv.at[r, u], device_id={"sp": to}, device_id_type=MESH)

    def result_arrival(r, u):
        source = device(chips - ahead(u), 0) if u < chips - 1 else partner
        at = r * n + source
        return pltpu.make_async_remote_copy(o_ref.at[at], o_ref.at[at], gsend.at[r, u], grecv.at[r, u], device_id={"sp": source}, device_id_type=MESH)

    def forward_copy(r, u):
        at = r * n + device(chips - ahead(u), 0)
        return pltpu.make_async_remote_copy(o_ref.at[at], o_ref.at[at], fsend.at[r, u], frecv.at[r, u], device_id={"sp": partner}, device_id_type=MESH)

    def forward_arrival(r, u):
        at = r * n + device(chips - ahead(u), 1)
        return pltpu.make_async_remote_copy(o_ref.at[at], o_ref.at[at], fsend.at[r, u], frecv.at[r, u], device_id={"sp": partner}, device_id_type=MESH)

    kcopy(0).start()
    qcopy = pltpu.make_async_copy(q_hbm, qv, qsem)
    qcopy.start()
    vcopy(0).start()
    for step in range(1, SLOTS):
        kcopy(step).start()
        vcopy(step).start()
    barrier = pltpu.get_barrier_semaphore()
    for far in range(1, n):
        pl.semaphore_signal(barrier, inc=1, device_id={"sp": lax.rem(me + far, n)}, device_id_type=MESH)
    for qb in (qb0, qb1):
        qb[...] = jnp.zeros(qb.shape, qb.dtype)

    def own_mask(rows):
        row = lax.rem(lax.broadcasted_iota(jnp.int32, (rows, LANES), 0), key_heads)
        lane = lax.rem(lax.broadcasted_iota(jnp.int32, (rows, LANES), 1), side)
        return (lane >= row * rep) & (lane < row * rep + rep)

    own8, own16 = own_mask(8), own_mask(16)

    def scores_start(step, qb):
        queries = qv[sequence(step)]
        qb[0:heads, 0:head] = queries
        qb[side : side + heads, head : 2 * head] = queries

    def scores_piece(step, piece, qb, s, high):
        slot = lax.rem(step, SLOTS)
        keys = jnp.concatenate([kbuf[slot, pl.ds(piece * CHUNK, CHUNK), :], kbuf[slot, pl.ds(half + piece * CHUNK, CHUNK), :]], axis=1)
        scores = lax.dot_general(keys, qb[...], (((1,), (1,)), ((), ())), preferred_element_type=F32)
        s[pl.ds(piece * CHUNK, CHUNK), :] = scores
        return jnp.maximum(high, jnp.max(scores.reshape(CHUNK // 8, 8, LANES), axis=0))

    def scores_end(high):
        high = jnp.max(jnp.where(own8, high, -jnp.inf), axis=0, keepdims=True)
        return jnp.maximum(high, pltpu.roll(high, side, 1))

    def values_piece(step, piece, s, high, total, seen):
        slot = lax.rem(step, SLOTS)
        weights = jnp.exp2(s[pl.ds(piece * CHUNK, CHUNK), :] * scale - high * scale)
        total = total + jnp.sum(weights.reshape(CHUNK // 8, 8, LANES), axis=0)
        rounded = weights.astype(BF16).reshape(CHUNK // 16, 16, LANES)
        rounded = jnp.where(own16[None], rounded, jnp.zeros_like(rounded)).reshape(CHUNK, LANES)
        values = jnp.concatenate([vbuf[slot, pl.ds(piece * CHUNK, CHUNK), :], vbuf[slot, pl.ds(half + piece * CHUNK, CHUNK), :]], axis=1)
        return total, seen + lax.dot_general(rounded, values, (((0,), (0,)), ((), ())), preferred_element_type=F32)

    def values_end(step, high, total, seen):
        total = jnp.sum(jnp.where(own8, total, 0.0), axis=0, keepdims=True)
        total = total + pltpu.roll(total, side, 1)
        seen = seen[0:heads, 0:head] + seen[side : side + heads, head : 2 * head]
        stage[step] = seen.astype(BF16)
        own_f[step // n] = seen
        stage_ml[step] = jnp.concatenate([high, total], axis=0)

    first = jnp.full((8, LANES), -jnp.inf, F32)
    zeros = (jnp.zeros((8, LANES), F32), jnp.zeros((2 * side, 2 * head), F32))

    def send(step):
        @pl.when(lax.rem(step, n) != n - 1)
        def _():
            for copy in part_copies(step):
                copy.start()

    def both(step, high, qb, s, s_before):
        scores_start(step, qb)
        new, (total, seen) = first, zeros
        for piece in range(pieces):
            new = scores_piece(step, piece, qb, s, new)
            total, seen = values_piece(step - 1, piece, s_before, high, total, seen)
        values_end(step - 1, high, total, seen)
        return scores_end(new)

    def refill(step):
        @pl.when(step + SLOTS < seqs)
        def _():
            kcopy(step + SLOTS).start()

        @pl.when(step - 1 + SLOTS < seqs)
        def _():
            vcopy(step - 1 + SLOTS).start()

    def combine(r):
        step = r * n + n - 1
        for t in range(n - 2):
            for copy in part_copies(r * n + t):
                copy.wait_recv()
        high = recv_ml[r, 0 : n - 2, 0, :]
        others = jnp.max(high, axis=0, keepdims=True)
        share = jnp.exp2(high * scale - others * scale)
        total = jnp.sum(share * recv_ml[r, 0 : n - 2, 1, :], axis=0, keepdims=True)
        share = jnp.concatenate([share, jnp.zeros((LANES - (n - 2), LANES), F32)], axis=0).T
        seen = share[0:heads, 0:1] * recv[r, 0].astype(F32)
        for t in range(1, n - 2):
            seen = seen + share[0:heads, t : t + 1] * recv[r, t].astype(F32)
        for copy in part_copies(r * n + n - 2):
            copy.wait_recv()
        high = jnp.concatenate([others, recv_ml[r, n - 2, 0:1, :], stage_ml[step, 0:1, :]], axis=0)
        total = jnp.concatenate([total, recv_ml[r, n - 2, 1:2, :], stage_ml[step, 1:2, :]], axis=0)
        share = jnp.exp2(high * scale - jnp.max(high, axis=0, keepdims=True) * scale)
        share = share / jnp.sum(share * total, axis=0, keepdims=True)
        share = jnp.concatenate([share, jnp.zeros((LANES - 3, LANES), F32)], axis=0).T
        seen = share[0:heads, 0:1] * seen + share[0:heads, 1:2] * recv[r, n - 2].astype(F32) + share[0:heads, 2:3] * own_f[r]
        o_ref[r * n + me] = seen.astype(BF16)
        for u in range(chips):
            result_copy(r, u).start()

    kcopy(0).wait()
    qcopy.wait()
    scores_start(0, qb0)
    high = first
    for piece in range(pieces):
        high = scores_piece(0, piece, qb0, s0, high)
    high = scores_end(high)
    kcopy(SLOTS).start()
    pl.semaphore_wait(barrier, n - 1)

    def body(trip, high):
        step = 2 * trip + 1
        kcopy(step).wait()
        vcopy(step - 1).wait()
        kcopy(step + 1).wait()
        vcopy(step).wait()
        high = both(step, high, qb1, s1, s0)
        high = both(step + 1, high, qb0, s0, s1)
        refill(step)
        refill(step + 1)

        @pl.when(trip >= 1)
        def _():
            send(step - 2)

        send(step - 1)
        for r in range(rounds - 1):
            @pl.when(step + 1 == (r + 1) * n + 4)
            def _():
                combine(r)

        return high

    high = lax.fori_loop(0, (seqs - 2) // 2, body, high)
    send(seqs - 3)
    kcopy(seqs - 1).wait()
    vcopy(seqs - 2).wait()
    high = both(seqs - 1, high, qb1, s1, s0)
    send(seqs - 2)
    vcopy(seqs - 1).wait()
    total, seen = zeros
    for piece in range(pieces):
        total, seen = values_piece(seqs - 1, piece, s1, high, total, seen)
    values_end(seqs - 1, high, total, seen)
    combine(rounds - 1)

    def drain(step, _):
        @pl.when(lax.rem(step, n) != n - 1)
        def _():
            for copy in part_copies(step):
                copy.wait_send()

        return 0

    lax.fori_loop(0, seqs, drain, 0)
    for r in range(rounds):
        for u in reversed(range(chips - 1)):
            result_arrival(r, u).wait_recv()
            forward_copy(r, u).start()
    for r in range(rounds):
        result_arrival(r, chips - 1).wait_recv()
        for u in range(chips):
            result_copy(r, u).wait_send()
        for u in range(chips - 1):
            forward_copy(r, u).wait_send()
            forward_arrival(r, u).wait_recv()


def solution(mesh):
    n = mesh.shape["sp"]

    def step(q, k, v):
        seqs, heads, head = q.shape
        tokens, key_heads = k.shape[1:3]
        rows = tokens * key_heads
        rounds = seqs // n
        in_hbm = pl.BlockSpec(memory_space=pltpu.HBM)
        dma = pltpu.SemaphoreType.DMA
        return pl.pallas_call(
            functools.partial(kernel, n, key_heads),
            out_shape=jax.ShapeDtypeStruct(q.shape, BF16),
            in_specs=[in_hbm] * 3,
            out_specs=pl.BlockSpec(memory_space=pltpu.VMEM),
            scratch_shapes=[
                pltpu.VMEM(q.shape, BF16),
                pltpu.VMEM((SLOTS, rows, head), BF16),
                pltpu.VMEM((SLOTS, rows, head), BF16),
                pltpu.VMEM((rows // 2, LANES), F32),
                pltpu.VMEM((rows // 2, LANES), F32),
                pltpu.VMEM((LANES, 2 * head), BF16),
                pltpu.VMEM((LANES, 2 * head), BF16),
                pltpu.VMEM((seqs, heads, head), BF16),
                pltpu.VMEM((seqs, 2, LANES), F32),
                pltpu.VMEM((rounds, heads, head), F32),
                pltpu.VMEM((rounds, n, heads, head), BF16),
                pltpu.VMEM((rounds, n, 2, LANES), F32),
                dma,
                dma((SLOTS,)),
                dma((SLOTS,)),
                dma((seqs,)),
                dma((rounds, n)),
                dma((seqs,)),
                dma((rounds, n)),
                dma((rounds, n // 2)),
                dma((rounds, n // 2)),
                dma((rounds, n // 2)),
                dma((rounds, n // 2)),
            ],
            compiler_params=pltpu.CompilerParams(collective_id=0, has_side_effects=True, vmem_limit_bytes=48 << 20),
        )(pltpu.with_memory_space_constraint(q, pltpu.HBM), k.reshape(seqs, rows, head), v.reshape(seqs, rows, head))

    return jax.shard_map(
        step,
        mesh=mesh,
        in_specs=(P("dp", None, None), P("dp", "sp", None, None), P("dp", "sp", None, None)),
        out_specs=P("dp", None, None),
        check_vma=False,
    )
```

```python
import functools
import math

import jax
import jax.numpy as jnp
from jax import lax
from jax.experimental import pallas as pl
from jax.experimental.pallas import tpu as pltpu
from jax.sharding import PartitionSpec as P

F32, BF16 = jnp.float32, jnp.bfloat16
MESH = pl.DeviceIdType.MESH
SLOTS = 6
CHUNK = 1024
LANES = 128


def kernel(n, key_heads, q_hbm, k_hbm, v_hbm, o_ref, qv, kbuf, vbuf, s0, s1, qb0, qb1, stage, stage_ml, own_f, recv, recv_ml,
           qsem, ksem, vsem, osend, orecv, msend, mrecv, gsend, grecv, fsend, frecv):
    seqs, heads, head = qv.shape
    rounds = seqs // n
    rep = heads // key_heads
    side = LANES // 2
    half = kbuf.shape[1] // 2
    pieces = half // CHUNK
    scale = head**-0.5 * math.log2(math.e)
    me = lax.axis_index("sp")

    chips = n // 2
    partner = 2 * (me // 2) + 1 - lax.rem(me, 2)

    def ahead(u):
        odd = u % 2
        return chips // 2 + (u // 2) * (1 - odd) - ((u + 1) // 2) * odd

    def device(dz, other):
        return 2 * lax.rem(me // 2 + dz, chips) + lax.rem(lax.rem(me, 2) + other, 2)

    def owner(step):
        t = lax.rem(step, n)
        return device(ahead(t // 2), 1 - lax.rem(t, 2))

    def sequence(step):
        return (step // n) * n + owner(step)

    def kcopy(step):
        slot = lax.rem(step, SLOTS)
        return pltpu.make_async_copy(k_hbm.at[sequence(step)], kbuf.at[slot], ksem.at[slot])

    def vcopy(step):
        slot = lax.rem(step, SLOTS)
        return pltpu.make_async_copy(v_hbm.at[sequence(step)], vbuf.at[slot], vsem.at[slot])

    def part_copies(step):
        to, r, t = owner(step), step // n, lax.rem(step, n)
        return (
            pltpu.make_async_remote_copy(stage.at[step], recv.at[r, t], osend.at[step], orecv.at[r, t], device_id={"sp": to}, device_id_type=MESH),
            pltpu.make_async_remote_copy(stage_ml.at[step], recv_ml.at[r, t], msend.at[step], mrecv.at[r, t], device_id={"sp": to}, device_id_type=MESH),
        )

    def result_copy(r, u):
        at = r * n + me
        to = device(ahead(u), 0) if u < chips - 1 else partner
        return pltpu.make_async_remote_copy(o_ref.at[at], o_ref.at[at], gsend.at[r, u], grecv.at[r, u], device_id={"sp": to}, device_id_type=MESH)

    def result_arrival(r, u):
        source = device(chips - ahead(u), 0) if u < chips - 1 else partner
        at = r * n + source
        return pltpu.make_async_remote_copy(o_ref.at[at], o_ref.at[at], gsend.at[r, u], grecv.at[r, u], device_id={"sp": source}, device_id_type=MESH)

    def forward_copy(r, u):
        at = r * n + device(chips - ahead(u), 0)
        return pltpu.make_async_remote_copy(o_ref.at[at], o_ref.at[at], fsend.at[r, u], frecv.at[r, u], device_id={"sp": partner}, device_id_type=MESH)

    def forward_arrival(r, u):
        at = r * n + device(chips - ahead(u), 1)
        return pltpu.make_async_remote_copy(o_ref.at[at], o_ref.at[at], fsend.at[r, u], frecv.at[r, u], device_id={"sp": partner}, device_id_type=MESH)

    qcopy = pltpu.make_async_copy(q_hbm, qv, qsem)
    qcopy.start()
    kcopy(0).start()
    kcopy(1).start()
    vcopy(0).start()
    barrier = pltpu.get_barrier_semaphore()
    for far in range(1, n):
        pl.semaphore_signal(barrier, inc=1, device_id={"sp": lax.rem(me + far, n)}, device_id_type=MESH)
    for qb in (qb0, qb1):
        qb[...] = jnp.zeros(qb.shape, qb.dtype)

    def own_mask(rows):
        row = lax.rem(lax.broadcasted_iota(jnp.int32, (rows, LANES), 0), key_heads)
        lane = lax.rem(lax.broadcasted_iota(jnp.int32, (rows, LANES), 1), side)
        return (lane >= row * rep) & (lane < row * rep + rep)

    own8, own16 = own_mask(8), own_mask(16)

    def scores_start(step, qb):
        queries = qv[sequence(step)]
        qb[0:heads, 0:head] = queries
        qb[side : side + heads, head : 2 * head] = queries

    def scores_piece(step, piece, qb, s, high):
        slot = lax.rem(step, SLOTS)
        keys = jnp.concatenate([kbuf[slot, pl.ds(piece * CHUNK, CHUNK), :], kbuf[slot, pl.ds(half + piece * CHUNK, CHUNK), :]], axis=1)
        scores = lax.dot_general(keys, qb[...], (((1,), (1,)), ((), ())), preferred_element_type=F32)
        s[pl.ds(piece * CHUNK, CHUNK), :] = scores
        return jnp.maximum(high, jnp.max(scores.reshape(CHUNK // 8, 8, LANES), axis=0))

    def scores_end(high):
        high = jnp.max(jnp.where(own8, high, -jnp.inf), axis=0, keepdims=True)
        return jnp.maximum(high, pltpu.roll(high, side, 1))

    def values_piece(step, piece, s, high, total, seen):
        slot = lax.rem(step, SLOTS)
        weights = jnp.exp2(s[pl.ds(piece * CHUNK, CHUNK), :] * scale - high * scale)
        total = total + jnp.sum(weights.reshape(CHUNK // 8, 8, LANES), axis=0)
        rounded = weights.astype(BF16).reshape(CHUNK // 16, 16, LANES)
        rounded = jnp.where(own16[None], rounded, jnp.zeros_like(rounded)).reshape(CHUNK, LANES)
        values = jnp.concatenate([vbuf[slot, pl.ds(piece * CHUNK, CHUNK), :], vbuf[slot, pl.ds(half + piece * CHUNK, CHUNK), :]], axis=1)
        return total, seen + lax.dot_general(rounded, values, (((0,), (0,)), ((), ())), preferred_element_type=F32)

    def values_end(step, high, total, seen):
        total = jnp.sum(jnp.where(own8, total, 0.0), axis=0, keepdims=True)
        total = total + pltpu.roll(total, side, 1)
        seen = seen[0:heads, 0:head] + seen[side : side + heads, head : 2 * head]
        stage[step] = seen.astype(BF16)
        own_f[step // n] = seen
        stage_ml[step] = jnp.concatenate([high, total], axis=0)

    first = jnp.full((8, LANES), -jnp.inf, F32)
    zeros = (jnp.zeros((8, LANES), F32), jnp.zeros((2 * side, 2 * head), F32))

    def send(step):
        @pl.when(lax.rem(step, n) != n - 1)
        def _():
            for copy in part_copies(step):
                copy.start()

    def both(step, high, qb, s, s_before):
        scores_start(step, qb)
        new, (total, seen) = first, zeros
        for piece in range(pieces):
            new = scores_piece(step, piece, qb, s, new)
            total, seen = values_piece(step - 1, piece, s_before, high, total, seen)
        values_end(step - 1, high, total, seen)
        return scores_end(new)

    def refill(step):
        for at in (step, step + 1):
            @pl.when(at < seqs)
            def _():
                kcopy(at).start()

            @pl.when(at - 1 < seqs)
            def _():
                vcopy(at - 1).start()

    def combine(r):
        step = r * n + n - 1
        for t in range(n - 2):
            for copy in part_copies(r * n + t):
                copy.wait_recv()
        high = recv_ml[r, 0 : n - 2, 0, :]
        others = jnp.max(high, axis=0, keepdims=True)
        share = jnp.exp2(high * scale - others * scale)
        total = jnp.sum(share * recv_ml[r, 0 : n - 2, 1, :], axis=0, keepdims=True)
        share = jnp.concatenate([share, jnp.zeros((LANES - (n - 2), LANES), F32)], axis=0).T
        seen = share[0:heads, 0:1] * recv[r, 0].astype(F32)
        for t in range(1, n - 2):
            seen = seen + share[0:heads, t : t + 1] * recv[r, t].astype(F32)
        for copy in part_copies(r * n + n - 2):
            copy.wait_recv()
        high = jnp.concatenate([others, recv_ml[r, n - 2, 0:1, :], stage_ml[step, 0:1, :]], axis=0)
        total = jnp.concatenate([total, recv_ml[r, n - 2, 1:2, :], stage_ml[step, 1:2, :]], axis=0)
        share = jnp.exp2(high * scale - jnp.max(high, axis=0, keepdims=True) * scale)
        share = share / jnp.sum(share * total, axis=0, keepdims=True)
        share = jnp.concatenate([share, jnp.zeros((LANES - 3, LANES), F32)], axis=0).T
        seen = share[0:heads, 0:1] * seen + share[0:heads, 1:2] * recv[r, n - 2].astype(F32) + share[0:heads, 2:3] * own_f[r]
        o_ref[r * n + me] = seen.astype(BF16)
        for u in range(chips):
            result_copy(r, u).start()

    kcopy(0).wait()
    qcopy.wait()
    for step in (2, 3, 4):
        kcopy(step).start()
        vcopy(step - 1).start()
    scores_start(0, qb0)
    high = first
    for piece in range(pieces):
        high = scores_piece(0, piece, qb0, s0, high)
    high = scores_end(high)
    pl.semaphore_wait(barrier, n - 1)

    def body(trip, high):
        step = 2 * trip + 1
        kcopy(step).wait()
        vcopy(step - 1).wait()
        kcopy(step + 1).wait()
        vcopy(step).wait()
        refill(step + 4)
        high = both(step, high, qb1, s1, s0)
        high = both(step + 1, high, qb0, s0, s1)

        @pl.when(trip >= 1)
        def _():
            send(step - 2)

        send(step - 1)
        for r in range(rounds - 1):
            @pl.when(step + 1 == (r + 1) * n + 4)
            def _():
                combine(r)

        return high

    high = lax.fori_loop(0, (seqs - 2) // 2, body, high)
    send(seqs - 3)
    kcopy(seqs - 1).wait()
    vcopy(seqs - 2).wait()
    high = both(seqs - 1, high, qb1, s1, s0)
    send(seqs - 2)
    vcopy(seqs - 1).wait()
    total, seen = zeros
    for piece in range(pieces):
        total, seen = values_piece(seqs - 1, piece, s1, high, total, seen)
    values_end(seqs - 1, high, total, seen)
    combine(rounds - 1)

    def drain(step, _):
        @pl.when(lax.rem(step, n) != n - 1)
        def _():
            for copy in part_copies(step):
                copy.wait_send()

        return 0

    lax.fori_loop(0, seqs, drain, 0)
    for r in range(rounds):
        for u in reversed(range(chips - 1)):
            result_arrival(r, u).wait_recv()
            forward_copy(r, u).start()
    for r in range(rounds):
        result_arrival(r, chips - 1).wait_recv()
        for u in range(chips):
            result_copy(r, u).wait_send()
        for u in range(chips - 1):
            forward_copy(r, u).wait_send()
            forward_arrival(r, u).wait_recv()


def solution(mesh):
    n = mesh.shape["sp"]

    def step(q, k, v):
        seqs, heads, head = q.shape
        tokens, key_heads = k.shape[1:3]
        rows = tokens * key_heads
        rounds = seqs // n
        in_hbm = pl.BlockSpec(memory_space=pltpu.HBM)
        dma = pltpu.SemaphoreType.DMA
        return pl.pallas_call(
            functools.partial(kernel, n, key_heads),
            out_shape=jax.ShapeDtypeStruct(q.shape, BF16),
            in_specs=[in_hbm] * 3,
            out_specs=pl.BlockSpec(memory_space=pltpu.VMEM),
            scratch_shapes=[
                pltpu.VMEM(q.shape, BF16),
                pltpu.VMEM((SLOTS, rows, head), BF16),
                pltpu.VMEM((SLOTS, rows, head), BF16),
                pltpu.VMEM((rows // 2, LANES), F32),
                pltpu.VMEM((rows // 2, LANES), F32),
                pltpu.VMEM((LANES, 2 * head), BF16),
                pltpu.VMEM((LANES, 2 * head), BF16),
                pltpu.VMEM((seqs, heads, head), BF16),
                pltpu.VMEM((seqs, 2, LANES), F32),
                pltpu.VMEM((rounds, heads, head), F32),
                pltpu.VMEM((rounds, n, heads, head), BF16),
                pltpu.VMEM((rounds, n, 2, LANES), F32),
                dma,
                dma((SLOTS,)),
                dma((SLOTS,)),
                dma((seqs,)),
                dma((rounds, n)),
                dma((seqs,)),
                dma((rounds, n)),
                dma((rounds, n // 2)),
                dma((rounds, n // 2)),
                dma((rounds, n // 2)),
                dma((rounds, n // 2)),
            ],
            compiler_params=pltpu.CompilerParams(collective_id=0, has_side_effects=True, vmem_limit_bytes=48 << 20),
        )(pltpu.with_memory_space_constraint(q, pltpu.HBM), k.reshape(seqs, rows, head), v.reshape(seqs, rows, head))

    return jax.shard_map(
        step,
        mesh=mesh,
        in_specs=(P("dp", None, None), P("dp", "sp", None, None), P("dp", "sp", None, None)),
        out_specs=P("dp", None, None),
        check_vma=False,
    )
```

```python
import functools
import math

import jax
import jax.numpy as jnp
from jax import lax
from jax.experimental import pallas as pl
from jax.experimental.pallas import tpu as pltpu
from jax.sharding import PartitionSpec as P

F32, BF16 = jnp.float32, jnp.bfloat16
MESH = pl.DeviceIdType.MESH
SLOTS = 8
CHUNK = 1024
LANES = 128


def rest(x, by):
    return x & (by - 1) if by & (by - 1) == 0 else lax.rem(x, by)


def whole(x, by):
    return x >> (by.bit_length() - 1) if by & (by - 1) == 0 else lax.div(x, by)


def kernel(n, key_heads, q_hbm, k_hbm, v_hbm, o_ref, qv, kbuf, vbuf, s0, s1, qb0, qb1, stage, stage_ml, own_f, recv, recv_ml,
           qsem, ksem, vsem, osend, orecv, msend, mrecv, gsend, grecv, fsend, frecv):
    seqs, heads, head = qv.shape
    rounds = seqs // n
    rep = heads // key_heads
    side = LANES // 2
    half = kbuf.shape[1] // 2
    pieces = half // CHUNK
    scale = head**-0.5 * math.log2(math.e)
    me = lax.axis_index("sp")

    chips = n // 2
    partner = me + 1 - 2 * rest(me, 2)

    def ahead(u):
        near, odd = (u // 2, u % 2) if isinstance(u, int) else (whole(u, 2), rest(u, 2))
        return chips // 2 + near - (2 * near + 1) * odd

    def device(dz, other):
        return 2 * rest(whole(me, 2) + dz, chips) + rest(rest(me, 2) + other, 2)

    def place(step):
        last = rounds * (n - 1)
        if isinstance(step, int):
            return (step // (n - 1), step % (n - 1)) if step < last else (step - last, n - 1)
        r = (step >= n - 1).astype(jnp.int32)
        own = (step >= last).astype(jnp.int32)
        return (1 - own) * r + own * (step - last), (1 - own) * (step - (n - 1) * r) + own * (n - 1)

    def owner(step):
        _, t = place(step)
        return device(ahead(whole(t, 2)), 1 - rest(t, 2))

    def sequence(step):
        return place(step)[0] * n + owner(step)

    def kcopy(step):
        slot = rest(step, SLOTS)
        return pltpu.make_async_copy(k_hbm.at[sequence(step)], kbuf.at[slot], ksem.at[slot])

    def vcopy(step):
        slot = rest(step, SLOTS)
        return pltpu.make_async_copy(v_hbm.at[sequence(step)], vbuf.at[slot], vsem.at[slot])

    def part_copies(step):
        (r, t), to = place(step), owner(step)
        return (
            pltpu.make_async_remote_copy(stage.at[step], recv.at[r, t], osend.at[step], orecv.at[r, t], device_id={"sp": to}, device_id_type=MESH),
            pltpu.make_async_remote_copy(stage_ml.at[step], recv_ml.at[r, t], msend.at[step], mrecv.at[r, t], device_id={"sp": to}, device_id_type=MESH),
        )

    def result_copy(r, u):
        at = r * n + me
        to = device(ahead(u), 0) if u < chips - 1 else partner
        return pltpu.make_async_remote_copy(o_ref.at[at], o_ref.at[at], gsend.at[r, u], grecv.at[r, u], device_id={"sp": to}, device_id_type=MESH)

    def result_arrival(r, u):
        source = device(chips - ahead(u), 0) if u < chips - 1 else partner
        at = r * n + source
        return pltpu.make_async_remote_copy(o_ref.at[at], o_ref.at[at], gsend.at[r, u], grecv.at[r, u], device_id={"sp": source}, device_id_type=MESH)

    def forward_copy(r, u):
        at = r * n + device(chips - ahead(u), 0)
        return pltpu.make_async_remote_copy(o_ref.at[at], o_ref.at[at], fsend.at[r, u], frecv.at[r, u], device_id={"sp": partner}, device_id_type=MESH)

    def forward_arrival(r, u):
        at = r * n + device(chips - ahead(u), 1)
        return pltpu.make_async_remote_copy(o_ref.at[at], o_ref.at[at], fsend.at[r, u], frecv.at[r, u], device_id={"sp": partner}, device_id_type=MESH)

    qcopy = pltpu.make_async_copy(q_hbm, qv, qsem)
    qcopy.start()
    kcopy(0).start()
    for step in (1, 2):
        kcopy(step).start()
        vcopy(step - 1).start()
    barrier = pltpu.get_barrier_semaphore()
    for far in range(1, n):
        pl.semaphore_signal(barrier, inc=1, device_id={"sp": lax.rem(me + far, n)}, device_id_type=MESH)
    for qb in (qb0, qb1):
        qb[...] = jnp.zeros(qb.shape, qb.dtype)

    def own_mask(rows):
        row = lax.rem(lax.broadcasted_iota(jnp.int32, (rows, LANES), 0), key_heads)
        lane = lax.rem(lax.broadcasted_iota(jnp.int32, (rows, LANES), 1), side)
        return (lane >= row * rep) & (lane < row * rep + rep)

    own8, own16 = own_mask(8), own_mask(16)

    def scores_start(step, qb):
        queries = qv[sequence(step)]
        qb[0:heads, 0:head] = queries
        qb[side : side + heads, head : 2 * head] = queries

    def scores_piece(step, piece, qb, s, high):
        slot = rest(step, SLOTS)
        keys = jnp.concatenate([kbuf[slot, pl.ds(piece * CHUNK, CHUNK), :], kbuf[slot, pl.ds(half + piece * CHUNK, CHUNK), :]], axis=1)
        scores = lax.dot_general(keys, qb[...], (((1,), (1,)), ((), ())), preferred_element_type=F32)
        s[pl.ds(piece * CHUNK, CHUNK), :] = scores
        return jnp.maximum(high, jnp.max(scores.reshape(CHUNK // 8, 8, LANES), axis=0))

    def scores_end(high):
        high = jnp.max(jnp.where(own8, high, -jnp.inf), axis=0, keepdims=True)
        return jnp.maximum(high, pltpu.roll(high, side, 1))

    def values_piece(step, piece, s, high, total, seen):
        slot = rest(step, SLOTS)
        weights = jnp.exp2(s[pl.ds(piece * CHUNK, CHUNK), :] * scale - high * scale)
        total = total + jnp.sum(weights.reshape(CHUNK // 8, 8, LANES), axis=0)
        rounded = weights.astype(BF16).reshape(CHUNK // 16, 16, LANES)
        rounded = jnp.where(own16[None], rounded, jnp.zeros_like(rounded)).reshape(CHUNK, LANES)
        values = jnp.concatenate([vbuf[slot, pl.ds(piece * CHUNK, CHUNK), :], vbuf[slot, pl.ds(half + piece * CHUNK, CHUNK), :]], axis=1)
        return total, seen + lax.dot_general(rounded, values, (((0,), (0,)), ((), ())), preferred_element_type=F32)

    def values_end(step, high, total, seen):
        total = jnp.sum(jnp.where(own8, total, 0.0), axis=0, keepdims=True)
        total = total + pltpu.roll(total, side, 1)
        seen = seen[0:heads, 0:head] + seen[side : side + heads, head : 2 * head]
        stage[step] = seen.astype(BF16)
        own_f[step & 1] = seen
        stage_ml[step] = jnp.concatenate([high, total], axis=0)

    first = jnp.full((8, LANES), -jnp.inf, F32)
    zeros = (jnp.zeros((8, LANES), F32), jnp.zeros((2 * side, 2 * head), F32))

    def send(step):
        @pl.when(step < rounds * (n - 1))
        def _():
            for copy in part_copies(step):
                copy.start()

    def both(step, high, qb, s, s_before):
        scores_start(step, qb)
        new, (total, seen) = first, zeros
        for piece in range(pieces):
            new = scores_piece(step, piece, qb, s, new)
            total, seen = values_piece(step - 1, piece, s_before, high, total, seen)
        values_end(step - 1, high, total, seen)
        return scores_end(new)

    def refill(step):
        for at in (step, step + 1):
            @pl.when(at < seqs)
            def _():
                kcopy(at).start()

            @pl.when(at - 1 < seqs)
            def _():
                vcopy(at - 1).start()

    def combine(r):
        step = rounds * (n - 1) + r
        for t in range(n - 2):
            for copy in part_copies(r * (n - 1) + t):
                copy.wait_recv()
        high = recv_ml[r, 0 : n - 2, 0, :]
        others = jnp.max(high, axis=0, keepdims=True)
        share = jnp.exp2(high * scale - others * scale)
        total = jnp.sum(share * recv_ml[r, 0 : n - 2, 1, :], axis=0, keepdims=True)
        share = jnp.concatenate([share, jnp.zeros((LANES - (n - 2), LANES), F32)], axis=0).T
        seen = share[0:heads, 0:1] * recv[r, 0].astype(F32)
        for t in range(1, n - 2):
            seen = seen + share[0:heads, t : t + 1] * recv[r, t].astype(F32)
        for copy in part_copies(r * (n - 1) + n - 2):
            copy.wait_recv()
        high = jnp.concatenate([others, recv_ml[r, n - 2, 0:1, :], stage_ml[step, 0:1, :]], axis=0)
        total = jnp.concatenate([total, recv_ml[r, n - 2, 1:2, :], stage_ml[step, 1:2, :]], axis=0)
        share = jnp.exp2(high * scale - jnp.max(high, axis=0, keepdims=True) * scale)
        share = share / jnp.sum(share * total, axis=0, keepdims=True)
        share = jnp.concatenate([share, jnp.zeros((LANES - 3, LANES), F32)], axis=0).T
        seen = share[0:heads, 0:1] * seen + share[0:heads, 1:2] * recv[r, n - 2].astype(F32) + share[0:heads, 2:3] * own_f[r]
        o_ref[r * n + me] = seen.astype(BF16)
        for u in range(chips):
            result_copy(r, u).start()

    kcopy(0).wait()
    qcopy.wait()
    for step in (3, 4, 5):
        kcopy(step).start()
        vcopy(step - 1).start()
    scores_start(0, qb0)
    high = first
    for piece in range(pieces):
        high = scores_piece(0, piece, qb0, s0, high)
    high = scores_end(high)
    pl.semaphore_wait(barrier, n - 1)

    def body(trip, high):
        step = 2 * trip + 1
        kcopy(step).wait()
        vcopy(step - 1).wait()
        kcopy(step + 1).wait()
        vcopy(step).wait()
        refill(step + 5)
        high = both(step, high, qb1, s1, s0)
        high = both(step + 1, high, qb0, s0, s1)

        @pl.when(trip >= 1)
        def _():
            send(step - 2)

        send(step - 1)
        return high

    high = lax.fori_loop(0, (seqs - 2) // 2, body, high)
    send(seqs - 3)
    kcopy(seqs - 1).wait()
    vcopy(seqs - 2).wait()
    high = both(seqs - 1, high, qb1, s1, s0)
    combine(0)
    vcopy(seqs - 1).wait()
    total, seen = zeros
    for piece in range(pieces):
        total, seen = values_piece(seqs - 1, piece, s1, high, total, seen)
    values_end(seqs - 1, high, total, seen)
    combine(rounds - 1)

    def drain(step, _):
        @pl.when(step < rounds * (n - 1))
        def _():
            for copy in part_copies(step):
                copy.wait_send()

        return 0

    lax.fori_loop(0, seqs, drain, 0)
    for r in range(rounds):
        for u in reversed(range(chips - 1)):
            result_arrival(r, u).wait_recv()
            forward_copy(r, u).start()
    for r in range(rounds):
        result_arrival(r, chips - 1).wait_recv()
        for u in range(chips):
            result_copy(r, u).wait_send()
        for u in range(chips - 1):
            forward_copy(r, u).wait_send()
            forward_arrival(r, u).wait_recv()


def solution(mesh):
    n = mesh.shape["sp"]

    def step(q, k, v):
        seqs, heads, head = q.shape
        tokens, key_heads = k.shape[1:3]
        rows = tokens * key_heads
        rounds = seqs // n
        in_hbm = pl.BlockSpec(memory_space=pltpu.HBM)
        dma = pltpu.SemaphoreType.DMA
        return pl.pallas_call(
            functools.partial(kernel, n, key_heads),
            out_shape=jax.ShapeDtypeStruct(q.shape, BF16),
            in_specs=[in_hbm] * 3,
            out_specs=pl.BlockSpec(memory_space=pltpu.VMEM),
            scratch_shapes=[
                pltpu.VMEM(q.shape, BF16),
                pltpu.VMEM((SLOTS, rows, head), BF16),
                pltpu.VMEM((SLOTS, rows, head), BF16),
                pltpu.VMEM((rows // 2, LANES), F32),
                pltpu.VMEM((rows // 2, LANES), F32),
                pltpu.VMEM((LANES, 2 * head), BF16),
                pltpu.VMEM((LANES, 2 * head), BF16),
                pltpu.VMEM((seqs, heads, head), BF16),
                pltpu.VMEM((seqs, 2, LANES), F32),
                pltpu.VMEM((rounds, heads, head), F32),
                pltpu.VMEM((rounds, n, heads, head), BF16),
                pltpu.VMEM((rounds, n, 2, LANES), F32),
                dma,
                dma((SLOTS,)),
                dma((SLOTS,)),
                dma((seqs,)),
                dma((rounds, n)),
                dma((seqs,)),
                dma((rounds, n)),
                dma((rounds, n // 2)),
                dma((rounds, n // 2)),
                dma((rounds, n // 2)),
                dma((rounds, n // 2)),
            ],
            compiler_params=pltpu.CompilerParams(collective_id=0, has_side_effects=True, vmem_limit_bytes=48 << 20),
        )(pltpu.with_memory_space_constraint(q, pltpu.HBM), k.reshape(seqs, rows, head), v.reshape(seqs, rows, head))

    return jax.shard_map(
        step,
        mesh=mesh,
        in_specs=(P("dp", None, None), P("dp", "sp", None, None), P("dp", "sp", None, None)),
        out_specs=P("dp", None, None),
        check_vma=False,
    )
```

```python
import functools
import math

import jax
import jax.numpy as jnp
from jax import lax
from jax.experimental import pallas as pl
from jax.experimental.pallas import tpu as pltpu
from jax.sharding import PartitionSpec as P

F32, BF16 = jnp.float32, jnp.bfloat16
MESH = pl.DeviceIdType.MESH
SLOTS = 8
CHUNK = 1024
LANES = 128
QUIET = 4


def rest(x, by):
    return x & (by - 1) if by & (by - 1) == 0 else lax.rem(x, by)


def whole(x, by):
    return x >> (by.bit_length() - 1) if by & (by - 1) == 0 else lax.div(x, by)


def kernel(n, key_heads, q_hbm, k_hbm, v_hbm, o_ref, qv, kbuf, vbuf, s0, s1, qb0, qb1, stage, stage_ml, own_f, recv, recv_ml,
           qsem, ksem, vsem, osend, orecv, msend, mrecv, gsend, grecv, fsend, frecv):
    seqs, heads, head = qv.shape
    rounds = seqs // n
    rep = heads // key_heads
    side = LANES // 2
    half = kbuf.shape[1] // 2
    pieces = half // CHUNK
    scale = head**-0.5 * math.log2(math.e)
    me = lax.axis_index("sp")

    chips = n // 2
    partner = me + 1 - 2 * rest(me, 2)

    def ahead(u):
        near, odd = (u // 2, u % 2) if isinstance(u, int) else (whole(u, 2), rest(u, 2))
        return chips // 2 + near - (2 * near + 1) * odd

    def device(dz, other):
        return 2 * rest(whole(me, 2) + dz, chips) + rest(rest(me, 2) + other, 2)

    def place(step):
        return (step % rounds, step // rounds) if isinstance(step, int) else (rest(step, rounds), whole(step, rounds))

    def owner(step):
        _, t = place(step)
        return device(ahead(t // 2 if isinstance(t, int) else whole(t, 2)), 1 - rest(t, 2))

    def sequence(step):
        return place(step)[0] * n + owner(step)

    def kcopy(step):
        slot = rest(step, SLOTS)
        return pltpu.make_async_copy(k_hbm.at[sequence(step)], kbuf.at[slot], ksem.at[slot])

    def vcopy(step):
        slot = rest(step, SLOTS)
        return pltpu.make_async_copy(v_hbm.at[sequence(step)], vbuf.at[slot], vsem.at[slot])

    def part_copies(t):
        to = owner(t * rounds)
        return (
            pltpu.make_async_remote_copy(stage.at[t], recv.at[t], osend.at[t], orecv.at[t], device_id={"sp": to}, device_id_type=MESH),
            pltpu.make_async_remote_copy(stage_ml.at[t], recv_ml.at[t], msend.at[t], mrecv.at[t], device_id={"sp": to}, device_id_type=MESH),
        )

    def result_copy(r, u):
        at = r * n + me
        to = device(ahead(u), 0) if u < chips - 1 else partner
        return pltpu.make_async_remote_copy(o_ref.at[at], o_ref.at[at], gsend.at[r, u], grecv.at[r, u], device_id={"sp": to}, device_id_type=MESH)

    def result_arrival(r, u):
        source = device(chips - ahead(u), 0) if u < chips - 1 else partner
        at = r * n + source
        return pltpu.make_async_remote_copy(o_ref.at[at], o_ref.at[at], gsend.at[r, u], grecv.at[r, u], device_id={"sp": source}, device_id_type=MESH)

    def forward_copy(r, u):
        at = r * n + device(chips - ahead(u), 0)
        return pltpu.make_async_remote_copy(o_ref.at[at], o_ref.at[at], fsend.at[r, u], frecv.at[r, u], device_id={"sp": partner}, device_id_type=MESH)

    def forward_arrival(r, u):
        at = r * n + device(chips - ahead(u), 1)
        return pltpu.make_async_remote_copy(o_ref.at[at], o_ref.at[at], fsend.at[r, u], frecv.at[r, u], device_id={"sp": partner}, device_id_type=MESH)

    qcopy = pltpu.make_async_copy(q_hbm, qv, qsem)
    qcopy.start()
    kcopy(0).start()
    for step in (1, 2):
        kcopy(step).start()
        vcopy(step - 1).start()
    barrier = pltpu.get_barrier_semaphore()
    for far in range(1, n):
        pl.semaphore_signal(barrier, inc=1, device_id={"sp": lax.rem(me + far, n)}, device_id_type=MESH)
    for qb in (qb0, qb1):
        qb[...] = jnp.zeros(qb.shape, qb.dtype)

    def own_mask(rows):
        row = lax.rem(lax.broadcasted_iota(jnp.int32, (rows, LANES), 0), key_heads)
        lane = lax.rem(lax.broadcasted_iota(jnp.int32, (rows, LANES), 1), side)
        return (lane >= row * rep) & (lane < row * rep + rep)

    own8, own16 = own_mask(8), own_mask(16)

    def scores_start(step, qb):
        queries = qv[sequence(step)]
        qb[0:heads, 0:head] = queries
        qb[side : side + heads, head : 2 * head] = queries

    def scores_piece(step, piece, qb, s, high):
        slot = rest(step, SLOTS)
        keys = jnp.concatenate([kbuf[slot, pl.ds(piece * CHUNK, CHUNK), :], kbuf[slot, pl.ds(half + piece * CHUNK, CHUNK), :]], axis=1)
        scores = lax.dot_general(keys, qb[...], (((1,), (1,)), ((), ())), preferred_element_type=F32)
        s[pl.ds(piece * CHUNK, CHUNK), :] = scores
        return jnp.maximum(high, jnp.max(scores.reshape(CHUNK // 8, 8, LANES), axis=0))

    def scores_end(high):
        high = jnp.max(jnp.where(own8, high, -jnp.inf), axis=0, keepdims=True)
        return jnp.maximum(high, pltpu.roll(high, side, 1))

    def values_piece(step, piece, s, high, total, seen):
        slot = rest(step, SLOTS)
        weights = jnp.exp2(s[pl.ds(piece * CHUNK, CHUNK), :] * scale - high * scale)
        total = total + jnp.sum(weights.reshape(CHUNK // 8, 8, LANES), axis=0)
        rounded = weights.astype(BF16).reshape(CHUNK // 16, 16, LANES)
        rounded = jnp.where(own16[None], rounded, jnp.zeros_like(rounded)).reshape(CHUNK, LANES)
        values = jnp.concatenate([vbuf[slot, pl.ds(piece * CHUNK, CHUNK), :], vbuf[slot, pl.ds(half + piece * CHUNK, CHUNK), :]], axis=1)
        return total, seen + lax.dot_general(rounded, values, (((0,), (0,)), ((), ())), preferred_element_type=F32)

    def values_end(step, high, total, seen):
        total = jnp.sum(jnp.where(own8, total, 0.0), axis=0, keepdims=True)
        total = total + pltpu.roll(total, side, 1)
        seen = seen[0:heads, 0:head] + seen[side : side + heads, head : 2 * head]
        r, t = place(step)
        stage[t, r] = seen.astype(BF16)
        own_f[r] = seen
        stage_ml[t, r] = jnp.concatenate([high, total], axis=0)

    first = jnp.full((8, LANES), -jnp.inf, F32)
    zeros = (jnp.zeros((8, LANES), F32), jnp.zeros((2 * side, 2 * head), F32))

    def send(t):
        for copy in part_copies(t):
            copy.start()

    def both(step, high, qb, s, s_before):
        scores_start(step, qb)
        new, (total, seen) = first, zeros
        for piece in range(pieces):
            new = scores_piece(step, piece, qb, s, new)
            total, seen = values_piece(step - 1, piece, s_before, high, total, seen)
        values_end(step - 1, high, total, seen)
        return scores_end(new)

    def refill(step):
        for at in (step, step + 1):
            @pl.when(at < seqs)
            def _():
                kcopy(at).start()

            @pl.when(at - 1 < seqs)
            def _():
                vcopy(at - 1).start()

    def far_parts(r):
        high = recv_ml[0 : n - 2, r, 0, :]
        highest = jnp.max(high, axis=0, keepdims=True)
        share = jnp.exp2(high * scale - highest * scale)
        total = jnp.sum(share * recv_ml[0 : n - 2, r, 1, :], axis=0, keepdims=True)
        share = jnp.concatenate([share, jnp.zeros((LANES - (n - 2), LANES), F32)], axis=0).T
        seen = share[0:heads, 0:1] * recv[0, r].astype(F32)
        for t in range(1, n - 2):
            seen = seen + share[0:heads, t : t + 1] * recv[t, r].astype(F32)
        return highest, total, seen

    def finish(r, high, total, seen):
        high = jnp.concatenate([high, recv_ml[n - 2, r, 0:1, :], stage_ml[n - 1, r, 0:1, :]], axis=0)
        total = jnp.concatenate([total, recv_ml[n - 2, r, 1:2, :], stage_ml[n - 1, r, 1:2, :]], axis=0)
        share = jnp.exp2(high * scale - jnp.max(high, axis=0, keepdims=True) * scale)
        share = share / jnp.sum(share * total, axis=0, keepdims=True)
        share = jnp.concatenate([share, jnp.zeros((LANES - 3, LANES), F32)], axis=0).T
        seen = share[0:heads, 0:1] * seen + share[0:heads, 1:2] * recv[n - 2, r].astype(F32) + share[0:heads, 2:3] * own_f[r]
        o_ref[r * n + me] = seen.astype(BF16)
        for u in range(chips):
            result_copy(r, u).start()

    kcopy(0).wait()
    qcopy.wait()
    for step in (3, 4, 5):
        kcopy(step).start()
        vcopy(step - 1).start()
    scores_start(0, qb0)
    high = first
    for piece in range(pieces):
        high = scores_piece(0, piece, qb0, s0, high)
    high = scores_end(high)

    def body(trip, high, sending):
        step = 2 * trip + 1
        kcopy(step).wait()
        vcopy(step - 1).wait()
        kcopy(step + 1).wait()
        vcopy(step).wait()
        refill(step + 5)

        if sending:
            send(trip - 1)

        high = both(step, high, qb1, s1, s0)
        high = both(step + 1, high, qb0, s0, s1)

        return high

    high = lax.fori_loop(0, QUIET, functools.partial(body, sending=False), high)
    pl.semaphore_wait(barrier, n - 1)
    for t in range(QUIET - 1):
        send(t)
    high = lax.fori_loop(QUIET, (seqs - 2) // 2, functools.partial(body, sending=True), high)
    send(n - 2)
    kcopy(seqs - 1).wait()
    vcopy(seqs - 2).wait()
    high = both(seqs - 1, high, qb1, s1, s0)
    for t in range(n - 2):
        for copy in part_copies(t):
            copy.wait_recv()
    parts = [far_parts(r) for r in range(rounds)]
    for copy in part_copies(n - 2):
        copy.wait_recv()
    for r in range(rounds - 1):
        finish(r, *parts[r])
    vcopy(seqs - 1).wait()
    total, seen = zeros
    for piece in range(pieces):
        total, seen = values_piece(seqs - 1, piece, s1, high, total, seen)
    values_end(seqs - 1, high, total, seen)
    finish(rounds - 1, *parts[-1])

    def drain(t, _):
        for copy in part_copies(t):
            copy.wait_send()
        return 0

    lax.fori_loop(0, n - 1, drain, 0)
    for r in range(rounds):
        for u in reversed(range(chips - 1)):
            result_arrival(r, u).wait_recv()
            forward_copy(r, u).start()
    for r in range(rounds):
        result_arrival(r, chips - 1).wait_recv()
        for u in range(chips):
            result_copy(r, u).wait_send()
        for u in range(chips - 1):
            forward_copy(r, u).wait_send()
            forward_arrival(r, u).wait_recv()


def solution(mesh):
    n = mesh.shape["sp"]

    def step(q, k, v):
        seqs, heads, head = q.shape
        tokens, key_heads = k.shape[1:3]
        rows = tokens * key_heads
        rounds = seqs // n
        in_hbm = pl.BlockSpec(memory_space=pltpu.HBM)
        dma = pltpu.SemaphoreType.DMA
        return pl.pallas_call(
            functools.partial(kernel, n, key_heads),
            out_shape=jax.ShapeDtypeStruct(q.shape, BF16),
            in_specs=[in_hbm] * 3,
            out_specs=pl.BlockSpec(memory_space=pltpu.VMEM),
            scratch_shapes=[
                pltpu.VMEM(q.shape, BF16),
                pltpu.VMEM((SLOTS, rows, head), BF16),
                pltpu.VMEM((SLOTS, rows, head), BF16),
                pltpu.VMEM((rows // 2, LANES), F32),
                pltpu.VMEM((rows // 2, LANES), F32),
                pltpu.VMEM((LANES, 2 * head), BF16),
                pltpu.VMEM((LANES, 2 * head), BF16),
                pltpu.VMEM((n, rounds, heads, head), BF16),
                pltpu.VMEM((n, rounds, 2, LANES), F32),
                pltpu.VMEM((rounds, heads, head), F32),
                pltpu.VMEM((n, rounds, heads, head), BF16),
                pltpu.VMEM((n, rounds, 2, LANES), F32),
                dma,
                dma((SLOTS,)),
                dma((SLOTS,)),
                dma((n,)),
                dma((n,)),
                dma((n,)),
                dma((n,)),
                dma((rounds, n // 2)),
                dma((rounds, n // 2)),
                dma((rounds, n // 2)),
                dma((rounds, n // 2)),
            ],
            compiler_params=pltpu.CompilerParams(collective_id=0, has_side_effects=True, vmem_limit_bytes=48 << 20),
        )(pltpu.with_memory_space_constraint(q, pltpu.HBM), k.reshape(seqs, rows, head), v.reshape(seqs, rows, head))

    return jax.shard_map(
        step,
        mesh=mesh,
        in_specs=(P("dp", None, None), P("dp", "sp", None, None), P("dp", "sp", None, None)),
        out_specs=P("dp", None, None),
        check_vma=False,
    )
```

```python
import functools
import math

import jax
import jax.numpy as jnp
from jax import lax
from jax.experimental import pallas as pl
from jax.experimental.pallas import tpu as pltpu
from jax.sharding import PartitionSpec as P

F32, BF16 = jnp.float32, jnp.bfloat16
MESH = pl.DeviceIdType.MESH
SLOTS = 8
CHUNK = 1024
LANES = 128
QUIET = 4


def rest(x, by):
    return x & (by - 1) if by & (by - 1) == 0 else lax.rem(x, by)


def whole(x, by):
    return x >> (by.bit_length() - 1) if by & (by - 1) == 0 else lax.div(x, by)


def kernel(n, key_heads, q_hbm, k_hbm, v_hbm, o_ref, qv, kbuf, vbuf, s0, s1, qb0, qb1, stage, stage_ml, own_f, recv, recv_ml,
           qsem, ksem, vsem, osend, orecv, msend, mrecv, gsend, grecv, fsend, frecv):
    seqs, heads, head = qv.shape
    rounds = seqs // n
    rep = heads // key_heads
    side = LANES // 2
    half = kbuf.shape[1] // 2
    pieces = half // CHUNK
    scale = head**-0.5 * math.log2(math.e)
    me = lax.axis_index("sp")

    chips = n // 2
    partner = me + 1 - 2 * rest(me, 2)

    def ahead(u):
        near, odd = (u // 2, u % 2) if isinstance(u, int) else (whole(u, 2), rest(u, 2))
        return chips // 2 - near + (2 * near + 1) * odd

    def device(dz, other):
        return 2 * rest(whole(me, 2) + dz, chips) + rest(rest(me, 2) + other, 2)

    def place(step):
        return (step % rounds, step // rounds) if isinstance(step, int) else (rest(step, rounds), whole(step, rounds))

    def owner(step):
        _, t = place(step)
        return device(ahead(t // 2 if isinstance(t, int) else whole(t, 2)), 1 - rest(t, 2))

    def sequence(step):
        return place(step)[0] * n + owner(step)

    def kcopy(step):
        slot = rest(step, SLOTS)
        return pltpu.make_async_copy(k_hbm.at[sequence(step)], kbuf.at[slot], ksem.at[slot])

    def vcopy(step):
        slot = rest(step, SLOTS)
        return pltpu.make_async_copy(v_hbm.at[sequence(step)], vbuf.at[slot], vsem.at[slot])

    def part_copies(t):
        to = owner(t * rounds)
        return (
            pltpu.make_async_remote_copy(stage.at[t], recv.at[t], osend.at[t], orecv.at[t], device_id={"sp": to}, device_id_type=MESH),
            pltpu.make_async_remote_copy(stage_ml.at[t], recv_ml.at[t], msend.at[t], mrecv.at[t], device_id={"sp": to}, device_id_type=MESH),
        )

    def result_copy(r, u):
        at = r * n + me
        to = device(ahead(u), 0) if u < chips - 1 else partner
        return pltpu.make_async_remote_copy(o_ref.at[at], o_ref.at[at], gsend.at[r, u], grecv.at[r, u], device_id={"sp": to}, device_id_type=MESH)

    def result_arrival(r, u):
        source = device(chips - ahead(u), 0) if u < chips - 1 else partner
        at = r * n + source
        return pltpu.make_async_remote_copy(o_ref.at[at], o_ref.at[at], gsend.at[r, u], grecv.at[r, u], device_id={"sp": source}, device_id_type=MESH)

    def forward_copy(r, u):
        at = r * n + device(chips - ahead(u), 0)
        return pltpu.make_async_remote_copy(o_ref.at[at], o_ref.at[at], fsend.at[r, u], frecv.at[r, u], device_id={"sp": partner}, device_id_type=MESH)

    def forward_arrival(r, u):
        at = r * n + device(chips - ahead(u), 1)
        return pltpu.make_async_remote_copy(o_ref.at[at], o_ref.at[at], fsend.at[r, u], frecv.at[r, u], device_id={"sp": partner}, device_id_type=MESH)

    qcopy = pltpu.make_async_copy(q_hbm, qv, qsem)
    qcopy.start()
    kcopy(0).start()
    for step in (1, 2):
        kcopy(step).start()
        vcopy(step - 1).start()
    barrier = pltpu.get_barrier_semaphore()
    for far in range(1, n):
        pl.semaphore_signal(barrier, inc=1, device_id={"sp": lax.rem(me + far, n)}, device_id_type=MESH)
    for qb in (qb0, qb1):
        qb[...] = jnp.zeros(qb.shape, qb.dtype)

    def own_mask(rows):
        row = lax.rem(lax.broadcasted_iota(jnp.int32, (rows, LANES), 0), key_heads)
        lane = lax.rem(lax.broadcasted_iota(jnp.int32, (rows, LANES), 1), side)
        return (lane >= row * rep) & (lane < row * rep + rep)

    own8, own16 = own_mask(8), own_mask(16)

    def scores_start(step, qb):
        queries = qv[sequence(step)]
        qb[0:heads, 0:head] = queries
        qb[side : side + heads, head : 2 * head] = queries

    def scores_piece(step, piece, qb, s, high):
        slot = rest(step, SLOTS)
        keys = jnp.concatenate([kbuf[slot, pl.ds(piece * CHUNK, CHUNK), :], kbuf[slot, pl.ds(half + piece * CHUNK, CHUNK), :]], axis=1)
        scores = lax.dot_general(keys, qb[...], (((1,), (1,)), ((), ())), preferred_element_type=F32)
        s[pl.ds(piece * CHUNK, CHUNK), :] = scores
        return jnp.maximum(high, jnp.max(scores.reshape(CHUNK // 8, 8, LANES), axis=0))

    def scores_end(high):
        high = jnp.max(jnp.where(own8, high, -jnp.inf), axis=0, keepdims=True)
        return jnp.maximum(high, pltpu.roll(high, side, 1))

    def values_piece(step, piece, s, high, total, seen):
        slot = rest(step, SLOTS)
        weights = jnp.exp2(s[pl.ds(piece * CHUNK, CHUNK), :] * scale - high * scale)
        total = total + jnp.sum(weights.reshape(CHUNK // 8, 8, LANES), axis=0)
        rounded = weights.astype(BF16).reshape(CHUNK // 16, 16, LANES)
        rounded = jnp.where(own16[None], rounded, jnp.zeros_like(rounded)).reshape(CHUNK, LANES)
        values = jnp.concatenate([vbuf[slot, pl.ds(piece * CHUNK, CHUNK), :], vbuf[slot, pl.ds(half + piece * CHUNK, CHUNK), :]], axis=1)
        return total, seen + lax.dot_general(rounded, values, (((0,), (0,)), ((), ())), preferred_element_type=F32)

    def values_end(step, high, total, seen):
        total = jnp.sum(jnp.where(own8, total, 0.0), axis=0, keepdims=True)
        total = total + pltpu.roll(total, side, 1)
        seen = seen[0:heads, 0:head] + seen[side : side + heads, head : 2 * head]
        r, t = place(step)
        stage[t, r] = seen.astype(BF16)
        own_f[r] = seen
        stage_ml[t, r] = jnp.concatenate([high, total], axis=0)

    first = jnp.full((8, LANES), -jnp.inf, F32)
    zeros = (jnp.zeros((8, LANES), F32), jnp.zeros((2 * side, 2 * head), F32))

    def send(t):
        for copy in part_copies(t):
            copy.start()

    def both(step, high, qb, s, s_before):
        scores_start(step, qb)
        new, (total, seen) = first, zeros
        for piece in range(pieces):
            new = scores_piece(step, piece, qb, s, new)
            total, seen = values_piece(step - 1, piece, s_before, high, total, seen)
        values_end(step - 1, high, total, seen)
        return scores_end(new)

    def refill(step):
        for at in (step, step + 1):
            @pl.when(at < seqs)
            def _():
                kcopy(at).start()

            @pl.when(at - 1 < seqs)
            def _():
                vcopy(at - 1).start()

    def far_parts(r):
        high = recv_ml[0 : n - 2, r, 0, :]
        highest = jnp.max(high, axis=0, keepdims=True)
        share = jnp.exp2(high * scale - highest * scale)
        total = jnp.sum(share * recv_ml[0 : n - 2, r, 1, :], axis=0, keepdims=True)
        share = jnp.concatenate([share, jnp.zeros((LANES - (n - 2), LANES), F32)], axis=0).T
        seen = share[0:heads, 0:1] * recv[0, r].astype(F32)
        for t in range(1, n - 2):
            seen = seen + share[0:heads, t : t + 1] * recv[t, r].astype(F32)
        return highest, total, seen

    def finish(r, high, total, seen):
        high = jnp.concatenate([high, recv_ml[n - 2, r, 0:1, :], stage_ml[n - 1, r, 0:1, :]], axis=0)
        total = jnp.concatenate([total, recv_ml[n - 2, r, 1:2, :], stage_ml[n - 1, r, 1:2, :]], axis=0)
        share = jnp.exp2(high * scale - jnp.max(high, axis=0, keepdims=True) * scale)
        share = share / jnp.sum(share * total, axis=0, keepdims=True)
        share = jnp.concatenate([share, jnp.zeros((LANES - 3, LANES), F32)], axis=0).T
        seen = share[0:heads, 0:1] * seen + share[0:heads, 1:2] * recv[n - 2, r].astype(F32) + share[0:heads, 2:3] * own_f[r]
        o_ref[r * n + me] = seen.astype(BF16)
        for u in range(chips):
            result_copy(r, u).start()

    kcopy(0).wait()
    qcopy.wait()
    for step in (3, 4, 5):
        kcopy(step).start()
        vcopy(step - 1).start()
    scores_start(0, qb0)
    high = first
    for piece in range(pieces):
        high = scores_piece(0, piece, qb0, s0, high)
    high = scores_end(high)

    def body(trip, high, sending):
        step = 2 * trip + 1
        kcopy(step).wait()
        vcopy(step - 1).wait()
        kcopy(step + 1).wait()
        vcopy(step).wait()
        refill(step + 5)

        if sending:
            send(trip - 1)

        high = both(step, high, qb1, s1, s0)
        high = both(step + 1, high, qb0, s0, s1)

        return high

    high = lax.fori_loop(0, QUIET, functools.partial(body, sending=False), high)
    pl.semaphore_wait(barrier, n - 1)
    for t in range(QUIET - 1):
        send(t)
    high = lax.fori_loop(QUIET, (seqs - 2) // 2, functools.partial(body, sending=True), high)
    send(n - 2)
    kcopy(seqs - 1).wait()
    vcopy(seqs - 2).wait()
    high = both(seqs - 1, high, qb1, s1, s0)
    for t in range(n - 2):
        for copy in part_copies(t):
            copy.wait_recv()
    parts = [far_parts(r) for r in range(rounds)]
    for copy in part_copies(n - 2):
        copy.wait_recv()
    for r in range(rounds - 1):
        finish(r, *parts[r])
    vcopy(seqs - 1).wait()
    total, seen = zeros
    for piece in range(pieces):
        total, seen = values_piece(seqs - 1, piece, s1, high, total, seen)
    values_end(seqs - 1, high, total, seen)
    finish(rounds - 1, *parts[-1])

    def drain(t, _):
        for copy in part_copies(t):
            copy.wait_send()
        return 0

    lax.fori_loop(0, n - 1, drain, 0)
    for r in range(rounds):
        for u in reversed(range(chips - 1)):
            result_arrival(r, u).wait_recv()
            forward_copy(r, u).start()
    for r in range(rounds):
        result_arrival(r, chips - 1).wait_recv()
        for u in range(chips):
            result_copy(r, u).wait_send()
        for u in range(chips - 1):
            forward_copy(r, u).wait_send()
            forward_arrival(r, u).wait_recv()


def solution(mesh):
    n = mesh.shape["sp"]

    def step(q, k, v):
        seqs, heads, head = q.shape
        tokens, key_heads = k.shape[1:3]
        rows = tokens * key_heads
        rounds = seqs // n
        in_hbm = pl.BlockSpec(memory_space=pltpu.HBM)
        dma = pltpu.SemaphoreType.DMA
        return pl.pallas_call(
            functools.partial(kernel, n, key_heads),
            out_shape=jax.ShapeDtypeStruct(q.shape, BF16),
            in_specs=[in_hbm] * 3,
            out_specs=pl.BlockSpec(memory_space=pltpu.VMEM),
            scratch_shapes=[
                pltpu.VMEM(q.shape, BF16),
                pltpu.VMEM((SLOTS, rows, head), BF16),
                pltpu.VMEM((SLOTS, rows, head), BF16),
                pltpu.VMEM((rows // 2, LANES), F32),
                pltpu.VMEM((rows // 2, LANES), F32),
                pltpu.VMEM((LANES, 2 * head), BF16),
                pltpu.VMEM((LANES, 2 * head), BF16),
                pltpu.VMEM((n, rounds, heads, head), BF16),
                pltpu.VMEM((n, rounds, 2, LANES), F32),
                pltpu.VMEM((rounds, heads, head), F32),
                pltpu.VMEM((n, rounds, heads, head), BF16),
                pltpu.VMEM((n, rounds, 2, LANES), F32),
                dma,
                dma((SLOTS,)),
                dma((SLOTS,)),
                dma((n,)),
                dma((n,)),
                dma((n,)),
                dma((n,)),
                dma((rounds, n // 2)),
                dma((rounds, n // 2)),
                dma((rounds, n // 2)),
                dma((rounds, n // 2)),
            ],
            compiler_params=pltpu.CompilerParams(collective_id=0, has_side_effects=True, vmem_limit_bytes=48 << 20),
        )(pltpu.with_memory_space_constraint(q, pltpu.HBM), k.reshape(seqs, rows, head), v.reshape(seqs, rows, head))

    return jax.shard_map(
        step,
        mesh=mesh,
        in_specs=(P("dp", None, None), P("dp", "sp", None, None), P("dp", "sp", None, None)),
        out_specs=P("dp", None, None),
        check_vma=False,
    )
```
